32 devices in a mesh: rows: 32 (over z, y, x, core).
Axes of the slice: x: 2, y: 2, z: 4, core: 2. Of those that a mesh axis runs over, the one named last changes fastest.
Arguments:
- q_final: float32 [49152, 512], P('rows'), may hold values from -0.084712684 to 0.084712684
- r_first: float32 [512, 512], replicated, may hold values from -1 to 2, as said below
- r_second: float32 [512, 512], replicated, may hold values from -1 to 2, as said below
- q_grad: float32 [49152, 512], P('rows'), may hold values from -6 to 6
- r_grad: float32 [512, 512], replicated, may hold values from -1.5 to 1.5
Outputs:
- a_grad: float32 [49152, 512], P('rows')
The draws below stay inside these ranges and needn't reach their ends.
Inputs may be any that keep to these rules, and one draw needn't show every extreme that they name: `r_first`: upper triangular, diagonal between 1 and 2. `r_second`: upper triangular, diagonal between 1 and 2.
All inputs are finite; a program needn't handle non-finite values.
Results may differ from the reference program's by a relative error of at most 0.000084.
Values sent between devices are 32-bit elements; how exact they have to be, the bound alone decides.
A program may use at most 128 MiB of HBM per device.

```python
import math
import jax
import jax.numpy as jnp
from jax import lax

W = 512
TOTAL = 49152


def triangle(key, salt):
    folded = jax.random.fold_in(key, salt)
    key_diag, key_off = jax.random.split(folded)
    diagonal = jnp.exp(jax.random.uniform(key_diag, (W,), jnp.float32, 0.0, math.log(2.0)))
    offdiag = jax.random.normal(key_off, (W, W), jnp.float32) * (0.25 / math.sqrt(W))
    return jnp.triu(offdiag, 1) + jnp.diag(diagonal)


def draw_r_first(key, part):
    return triangle(key, 11)


def draw_r_second(key, part):
    return triangle(key, 23)


def shard_levels(own_key, extent, cuts, smallest, top_value):
    factor_of, own = 1.0, jax.random.fold_in(own_key, 6)
    for position, blocks in cuts:
        draws = jnp.exp(jax.random.uniform(jax.random.fold_in(own, position), (blocks,), jnp.float32, smallest / len(cuts), top_value / len(cuts)))
        factor_of = factor_of * jnp.repeat(draws, extent[position] // blocks).reshape([-1 if axis == position else 1 for axis in range(len(extent))])
    return factor_of


def noise(key, extent, width, limit, cuts=(), held_as=jnp.bfloat16):
    result = width * jax.random.normal(key, extent, jnp.float32)
    if cuts:
        result = result * shard_levels(key, extent, cuts, -0.22, 0.18)
    return jnp.clip(result, -limit, limit).astype(held_as)


def setup_inputs(seed: int = 0) -> dict:
    key_of = jax.random.split(jax.random.key(seed), 6)
    q_final = noise(key_of[0], (TOTAL, W), ((TOTAL * W) ** -0.25), 0.084712684, ((0, 32),), jnp.float32)
    r_first = draw_r_first(jax.random.fold_in(key_of[5], 71), 0)
    r_second = draw_r_second(jax.random.fold_in(key_of[5], 71), 0)
    q_grad = noise(key_of[3], (TOTAL, W), 1.0, 6.0, ((0, 32),), jnp.float32)
    r_grad = noise(key_of[4], (W, W), 0.25, 1.5, (), jnp.float32)
    return {"q_final": q_final, "r_first": r_first, "r_second": r_second, "q_grad": q_grad, "r_grad": r_grad}


HIGHEST = lax.Precision.HIGHEST

def copy_lower(matrix):
    return jnp.tril(matrix) + jnp.tril(matrix, -1).T

def right_solve(left, upper):
    return lax.linalg.triangular_solve(upper, left, left_side=False, lower=False, transpose_a=True)

def reference(q_final, r_first, r_second, q_grad, r_grad):
    q_first = jnp.dot(q_final, r_second, precision=HIGHEST)
    grad_second = jnp.dot(r_grad, r_first.T, precision=HIGHEST)
    grad_first = jnp.dot(r_second.T, r_grad, precision=HIGHEST)
    mix_second = jnp.dot(r_second, grad_second.T, precision=HIGHEST) - jnp.dot(q_grad.T, q_final, precision=HIGHEST)
    inner = q_grad + jnp.dot(q_final, copy_lower(mix_second), precision=HIGHEST)
    q_first_grad = right_solve(inner, r_second)
    mix_first = jnp.dot(r_first, grad_first.T, precision=HIGHEST) - jnp.dot(q_first_grad.T, q_first, precision=HIGHEST)
    outer = q_first_grad + jnp.dot(q_first, copy_lower(mix_first), precision=HIGHEST)
    return right_solve(outer, r_first)
```

```python
import functools

import jax
import jax.numpy as jnp
from jax import lax
from jax.experimental import pallas as pl
from jax.experimental.pallas import tpu as pltpu
from jax.sharding import PartitionSpec as P

HIGH = lax.Precision.HIGH
MESH = pl.DeviceIdType.MESH
LANES = 128
FULL_ROWS = 96
VMEM_BYTES = 56 * 1024 * 1024


def iota2(shape):
    return lax.broadcasted_iota(jnp.int32, shape, 0), lax.broadcasted_iota(jnp.int32, shape, 1)


def split(x):
    high = x.astype(jnp.bfloat16)
    return high, (x - high.astype(jnp.float32)).astype(jnp.bfloat16)


def mm(a, b, dims=((1,), (0,))):
    a_high, a_low = split(a)
    b_high, b_low = split(b)
    dot = functools.partial(
        lax.dot_general, dimension_numbers=(dims, ((), ())), preferred_element_type=jnp.float32
    )
    return dot(a_high, b_high) + (dot(a_high, b_low) + dot(a_low, b_high))


NT = ((1,), (1,))


def base_inverses(blocks):
    order = blocks[0].shape[0]
    row, col = iota2((order, order))
    eye = row == col
    inverses = [jnp.where(eye, 1.0 / jnp.where(eye, block, 1.0), 0.0) for block in blocks]
    span = 1
    while span < order:
        mask = (row // (2 * span) == col // (2 * span)) & (row // span < col // span)
        right = [mm(jnp.where(mask, b, 0.0), i) for b, i in zip(blocks, inverses)]
        inverses = [i - mm(i, r) for i, r in zip(inverses, right)]
        span *= 2
    return inverses


def invert(uppers, outs):
    order = uppers[0].shape[0]
    base = LANES if order % LANES == 0 else order
    for out in outs:
        out[...] = jnp.zeros_like(out)
    spots = [(m, s) for m in range(len(uppers)) for s in range(0, order, base)]
    blocks = base_inverses([uppers[m][s : s + base, s : s + base] for m, s in spots])
    for (m, s), block in zip(spots, blocks):
        outs[m][s : s + base, s : s + base] = block
    span = base
    while span < order:
        work = []
        for m in range(len(uppers)):
            for s in range(0, order - span, 2 * span):
                e = min(s + 2 * span, order)
                right = mm(uppers[m][s : s + span, s + span : e], outs[m][s + span : e, s + span : e])
                work.append((m, s, e, right))
        for m, s, e, right in work:
            outs[m][s : s + span, s + span : e] = -mm(outs[m][s : s + span, s : s + span], right)
        span *= 2


def small_kernel(r1, r2, rg, inv1, inv2, v_out, h_out, e_out):
    invert((r1, r2), (inv1, inv2))
    v_out[...] = mm(inv1[...], inv2[...])
    w = mm(r1[...], rg[...], NT)
    h_out[...] = mm(r2[...], w)
    e_out[...] = mm(w, r2[...])


def plan(n, rows):
    bits = list(range(n.bit_length() - 1))
    rest = bits[1:]
    half = len(rest) // 2
    swapped = [rest[i ^ 1] if (i ^ 1) < len(rest) else rest[i] for i in range(len(rest))]
    orders = [rest, swapped, rest[half:] + rest[:half]]
    unit = rows // 8
    sizes = [3 * unit, 3 * unit, rows - 6 * unit]
    out, start = [], 0
    for order, size in zip(orders, sizes):
        out.append((start, size, bits[:1] + order))
        start += size
    return out


def reduce_kernel(n, p_ref, d_ref, out_ref, dout_ref, acc, recv, gat, dacc, drecv, send_sem, recv_sem, dsend, drecv_sem):
    me = lax.axis_index("rows")
    levels = n.bit_length() - 1
    order, width = p_ref.shape

    def partner(bit):
        step = 1 << bit
        return me + step * (1 - 2 * ((me // step) % 2))

    barrier = pltpu.get_barrier_semaphore()
    for bit in range(levels):
        pl.semaphore_signal(barrier, inc=1, device_id=(partner(bit),), device_id_type=MESH)
    pl.semaphore_wait(barrier, levels)

    for j in range(width // LANES):
        acc[j * order : (j + 1) * order, :] = p_ref[:, j * LANES : (j + 1) * LANES]
    dacc[0] = d_ref[...]

    streams = plan(n, acc.shape[0])
    state = [(start, size) for start, size, _ in streams]
    base = [0] * len(streams)
    slot0 = 0
    for i, (_, size, _) in enumerate(streams):
        base[i] = slot0
        slot0 += 2 * size
    trail = [[] for _ in streams]

    def at(ref, off, size):
        return ref.at[pl.ds(pl.multiple_of(off, 8), size), :]

    for k in range(levels):
        pending = []
        for i, (_, _, bits) in enumerate(streams):
            off, size = state[i]
            peer = partner(bits[k])
            mine = (me // (1 << bits[k])) % 2
            halve = (size // 2) % 8 == 0 and size > FULL_ROWS
            part = size // 2 if halve else size
            send_off = off + (1 - mine) * part if halve else off
            keep_off = off + mine * part if halve else off
            landing = recv.at[pl.ds(base[i], part), :]
            copy = pltpu.make_async_remote_copy(
                src_ref=at(acc, send_off, part), dst_ref=landing,
                send_sem=send_sem.at[i, k], recv_sem=recv_sem.at[i, k],
                device_id=(peer,), device_id_type=MESH,
            )
            copy.start()
            pending.append((i, copy, keep_off, part, landing))
            if halve:
                trail[i].append((peer, off, keep_off, part))
            base[i] += part
            state[i] = (keep_off, part)
        dcopy = pltpu.make_async_remote_copy(
            src_ref=dacc.at[k], dst_ref=drecv.at[k], send_sem=dsend.at[k], recv_sem=drecv_sem.at[k],
            device_id=(partner(k),), device_id_type=MESH,
        )
        dcopy.start()
        for i, copy, keep_off, part, landing in pending:
            copy.wait()
            target = acc if k < levels - 1 else gat
            rows = pl.ds(pl.multiple_of(keep_off, 8), part)
            target[rows, :] = acc[rows, :] + landing[...]
        dcopy.wait()
        dacc[k + 1] = dacc[k] + drecv[k]

    depth = max(len(t) for t in trail)
    for back in range(depth):
        pending = []
        for i in range(len(streams)):
            if back >= len(trail[i]):
                continue
            peer, _, keep_off, part = trail[i][len(trail[i]) - 1 - back]
            copy = pltpu.make_async_remote_copy(
                src_ref=at(gat, keep_off, part), dst_ref=at(gat, keep_off, part),
                send_sem=send_sem.at[i, levels + back], recv_sem=recv_sem.at[i, levels + back],
                device_id=(peer,), device_id_type=MESH,
            )
            copy.start()
            pending.append(copy)
        for copy in pending:
            copy.wait()

    for j in range(width // LANES):
        out_ref[:, j * LANES : (j + 1) * LANES] = gat[j * order : (j + 1) * order, :]
    dout_ref[...] = dacc[levels]


def all_sum(n, packed, diag):
    levels = n.bit_length() - 1
    if n != 1 << levels or n < 4:
        return lax.psum((packed, diag), "rows")
    rows = packed.size // LANES
    vmem = pl.BlockSpec(memory_space=pltpu.VMEM)
    return pl.pallas_call(
        functools.partial(reduce_kernel, n),
        out_shape=(
            jax.ShapeDtypeStruct(packed.shape, jnp.float32),
            jax.ShapeDtypeStruct(diag.shape, jnp.float32),
        ),
        in_specs=[vmem, vmem],
        out_specs=(vmem, vmem),
        scratch_shapes=[
            pltpu.VMEM((rows, LANES), jnp.float32),
            pltpu.VMEM((2 * rows, LANES), jnp.float32),
            pltpu.VMEM((rows, LANES), jnp.float32),
            pltpu.VMEM((levels + 1,) + diag.shape, jnp.float32),
            pltpu.VMEM((levels,) + diag.shape, jnp.float32),
            pltpu.SemaphoreType.DMA((3, 2 * levels)),
            pltpu.SemaphoreType.DMA((3, 2 * levels)),
            pltpu.SemaphoreType.DMA((levels,)),
            pltpu.SemaphoreType.DMA((levels,)),
        ],
        compiler_params=pltpu.CompilerParams(
            collective_id=0, has_side_effects=True, vmem_limit_bytes=VMEM_BYTES
        ),
        name="reduce",
    )(packed, diag)


def dot(a, b):
    return jnp.dot(a, b, precision=HIGH)


def dot_nt(a, b):
    return lax.dot_general(a, b, (((1,), (1,)), ((), ())), precision=HIGH)


def cross_product(left, right):
    return lax.dot_general(left, right, (((0,), (0,)), ((), ())), precision=HIGH)


def copy_lower(matrix):
    return jnp.tril(matrix) + jnp.tril(matrix, -1).T


def local(n, q_final, r_first, r_second, q_grad, r_grad):
    width = q_final.shape[1]
    row, col = iota2((width, width))
    lower = row >= col
    packed = jnp.where(lower, cross_product(q_grad, q_final), cross_product(q_final, q_final))
    diag = jnp.broadcast_to(jnp.sum(q_final * q_final, axis=0)[None, :], (8, width))
    vmem = pl.BlockSpec(memory_space=pltpu.VMEM)
    square = jax.ShapeDtypeStruct((width, width), jnp.float32)
    inv1, inv2, v, h, e = pl.pallas_call(
        small_kernel,
        out_shape=(square,) * 5,
        in_specs=[vmem] * 3,
        out_specs=(vmem,) * 5,
        compiler_params=pltpu.CompilerParams(vmem_limit_bytes=VMEM_BYTES),
        name="small",
    )(r_first, r_second, r_grad)
    packed, diag = all_sum(n, packed, diag)
    upper = jnp.where(row < col, packed, 0.0)
    gram = upper + upper.T + jnp.where(row == col, diag[0][None, :], 0.0)
    cross = jnp.where(lower, packed, 0.0)
    second_copy = copy_lower(h - cross)
    middle = jnp.tril(cross + dot(second_copy, gram))
    first_copy = copy_lower(e - dot(dot(inv2, middle), r_second))
    weight = dot_nt(second_copy, v) + dot_nt(dot(r_second, first_copy), inv1)
    return dot_nt(q_grad, v) + dot(q_final, weight)


def solution(mesh):
    n = mesh.shape["rows"]
    placed = (P("rows", None), P(), P(), P("rows", None), P())
    return jax.shard_map(
        functools.partial(local, n), mesh=mesh, in_specs=placed, out_specs=P("rows", None), check_vma=False
    )
```

```python
import functools

import jax
import jax.numpy as jnp
from jax import lax
from jax.experimental import pallas as pl
from jax.experimental.pallas import tpu as pltpu
from jax.sharding import PartitionSpec as P

MESH = pl.DeviceIdType.MESH
LANES = 128
FULL_ROWS = 96
VMEM_BYTES = 56 * 1024 * 1024


def iota2(shape):
    return lax.broadcasted_iota(jnp.int32, shape, 0), lax.broadcasted_iota(jnp.int32, shape, 1)


def split(x):
    high = x.astype(jnp.bfloat16)
    return high, (x - high.astype(jnp.float32)).astype(jnp.bfloat16)


def mm(a, b, dims=((1,), (0,))):
    a_high, a_low = split(a)
    b_high, b_low = split(b)
    dot = functools.partial(
        lax.dot_general, dimension_numbers=(dims, ((), ())), preferred_element_type=jnp.float32
    )
    return dot(a_high, b_high) + (dot(a_high, b_low) + dot(a_low, b_high))


NT = ((1,), (1,))


TN = ((0,), (0,))


def inverse_steps(uppers, outs):
    order = uppers[0].shape[0]
    base = LANES if order % LANES == 0 else order
    spots = [(m, slice(s, s + base)) for m in range(len(uppers)) for s in range(0, order, base)]

    def init():
        row, col = iota2((base, base))
        eye = row == col
        for out in outs:
            out[...] = jnp.zeros_like(out)
        for m, s in spots:
            outs[m][s, s] = jnp.where(eye, 1.0 / jnp.where(eye, uppers[m][s, s], 1.0), 0.0)

    def inner(span):
        row, col = iota2((base, base))
        mask = (row // (2 * span) == col // (2 * span)) & (row // span < col // span)
        blocks = [outs[m][s, s] for m, s in spots]
        right = [mm(jnp.where(mask, uppers[m][s, s], 0.0), i) for (m, s), i in zip(spots, blocks)]
        for (m, s), i, r in zip(spots, blocks, right):
            outs[m][s, s] = i - mm(i, r)

    def corner(span):
        work = []
        for m in range(len(uppers)):
            for s in range(0, order - span, 2 * span):
                top, low = slice(s, s + span), slice(s + span, min(s + 2 * span, order))
                work.append((m, top, low, mm(uppers[m][top, low], outs[m][low, low])))
        for m, top, low, right in work:
            outs[m][top, low] = -mm(outs[m][top, top], right)

    steps, span = [init], 1
    while span < order:
        steps.append(functools.partial(inner if span < base else corner, span))
        span *= 2
    return steps


def small_steps(r1, r2, rg, inv1, inv2, w, h, e, vh, vl):
    def first():
        w[...] = mm(r1[...], rg[...], NT)

    def second():
        h[...] = mm(r2[...], w[...])

    def third():
        e[...] = mm(w[...], r2[...])

    def fourth():
        vh[...], vl[...] = split(mm(inv1[...], inv2[...]).T)

    return [first, second, third] + inverse_steps((r1, r2), (inv1, inv2)) + [fourth]


def copy_lower(matrix):
    row, col = iota2(matrix.shape)
    return jnp.where(row >= col, matrix, 0.0) + jnp.where(row > col, matrix, 0.0).T


def tail(packed, diag, r2, inv1, inv2, h, e, vh, vl, gram, second, third, bh, bl):
    row, col = iota2(packed.shape)
    upper = jnp.where(row < col, packed[...], 0.0)
    gram[...] = upper + upper.T + jnp.where(row == col, diag[0:1, :], 0.0)
    second[...] = copy_lower(h[...] - packed[...])
    third[...] = packed[...] + mm(second[...], gram[...])
    third[...] = mm(inv2[...], jnp.where(row >= col, third[...], 0.0))
    third[...] = copy_lower(e[...] - mm(third[...], r2[...]))
    third[...] = mm(r2[...], third[...])
    third[...] = mm(third[...], inv1[...], NT)
    s_high, s_low = split(second[...])
    dot = functools.partial(jnp.dot, preferred_element_type=jnp.float32)
    third[...] += dot(s_high, vh[...]) + (dot(s_high, vl[...]) + dot(s_low, vh[...]))
    bh[...], bl[...] = split(third[...])


def gram_kernel(q_ref, g_ref, out_ref, diag_ref, cross, gram):
    step = pl.program_id(0)

    @pl.when(step == 0)
    def _():
        cross[...] = jnp.zeros_like(cross)
        gram[...] = jnp.zeros_like(gram)

    half = q_ref.shape[1] // 2
    low, top = slice(0, half), slice(half, 2 * half)
    q1, q2, g1, g2 = q_ref[:, low], q_ref[:, top], g_ref[:, low], g_ref[:, top]
    q1, q2, g1, g2 = split(q1), split(q2), split(g1), split(g2)

    def product(a, b):
        dot = functools.partial(
            lax.dot_general, dimension_numbers=(TN, ((), ())), preferred_element_type=jnp.float32
        )
        return dot(a[0], b[0]) + (dot(a[0], b[1]) + dot(a[1], b[0]))

    cross[low, low] += product(g1, q1)
    cross[top, low] += product(g2, q1)
    cross[top, top] += product(g2, q2)
    gram[low, low] += product(q1, q1)
    gram[low, top] += product(q1, q2)
    gram[top, top] += product(q2, q2)

    @pl.when(step == pl.num_programs(0) - 1)
    def _():
        row, col = iota2(out_ref.shape)
        out_ref[...] = jnp.where(row >= col, cross[...], gram[...])
        line = jnp.sum(jnp.where(row == col, gram[...], 0.0), axis=0, keepdims=True)
        diag_ref[...] = jnp.broadcast_to(line, diag_ref.shape)


def last_kernel(q_ref, g_ref, vh, vl, bh, bl, out_ref):
    g_high, g_low = split(g_ref[...])
    q_high, q_low = split(q_ref[...])
    dot = functools.partial(jnp.dot, preferred_element_type=jnp.float32)
    out_ref[...] = (dot(g_high, vh[...]) + dot(q_high, bh[...])) + (
        (dot(g_high, vl[...]) + dot(g_low, vh[...])) + (dot(q_high, bl[...]) + dot(q_low, bh[...]))
    )


def plan(n, rows):
    bits = list(range(n.bit_length() - 1))
    rest = bits[1:]
    half = len(rest) // 2
    swapped = [rest[i ^ 1] if (i ^ 1) < len(rest) else rest[i] for i in range(len(rest))]
    orders = [rest, swapped, rest[half:] + rest[:half]]
    unit = rows // 8
    sizes = [3 * unit, 3 * unit, rows - 6 * unit]
    out, start = [], 0
    for order, size in zip(orders, sizes):
        out.append((start, size, bits[:1] + order))
        start += size
    return out


def reduce_kernel(
    n, p_ref, d_ref, r1, r2, rg, vh, vl, bh, bl,
    total, inv1, inv2, w, h, e, gram, second, third,
    acc, recv, gat, dacc, drecv, send_sem, recv_sem, dsend, drecv_sem,
):
    me = lax.axis_index("rows")
    levels = n.bit_length() - 1
    order, width = p_ref.shape

    def partner(bit):
        step = 1 << bit
        return me + step * (1 - 2 * ((me // step) % 2))

    barrier = pltpu.get_barrier_semaphore()
    for bit in range(levels):
        pl.semaphore_signal(barrier, inc=1, device_id=(partner(bit),), device_id_type=MESH)
    pl.semaphore_wait(barrier, levels)

    for j in range(width // LANES):
        acc[j * order : (j + 1) * order, :] = p_ref[:, j * LANES : (j + 1) * LANES]
    dacc[0] = d_ref[...]

    streams = plan(n, acc.shape[0])
    steps = small_steps(r1, r2, rg, inv1, inv2, w, h, e, vh, vl)

    def fill(count):
        for _ in range(min(count, len(steps))):
            steps.pop(0)()

    state = [(start, size) for start, size, _ in streams]
    base = [0] * len(streams)
    slot0 = 0
    for i, (_, size, _) in enumerate(streams):
        base[i] = slot0
        slot0 += 2 * size
    trail = [[] for _ in streams]

    def at(ref, off, size):
        return ref.at[pl.ds(pl.multiple_of(off, 8), size), :]

    for k in range(levels):
        pending = []
        for i, (_, _, bits) in enumerate(streams):
            off, size = state[i]
            peer = partner(bits[k])
            mine = (me // (1 << bits[k])) % 2
            halve = (size // 2) % 8 == 0 and size > FULL_ROWS
            part = size // 2 if halve else size
            send_off = off + (1 - mine) * part if halve else off
            keep_off = off + mine * part if halve else off
            landing = recv.at[pl.ds(base[i], part), :]
            copy = pltpu.make_async_remote_copy(
                src_ref=at(acc, send_off, part), dst_ref=landing,
                send_sem=send_sem.at[i, k], recv_sem=recv_sem.at[i, k],
                device_id=(peer,), device_id_type=MESH,
            )
            copy.start()
            pending.append((i, copy, keep_off, part, landing))
            if halve:
                trail[i].append((peer, off, keep_off, part))
            base[i] += part
            state[i] = (keep_off, part)
        dcopy = pltpu.make_async_remote_copy(
            src_ref=dacc.at[k], dst_ref=drecv.at[k], send_sem=dsend.at[k], recv_sem=drecv_sem.at[k],
            device_id=(partner(k),), device_id_type=MESH,
        )
        dcopy.start()
        fill(2)
        for i, copy, keep_off, part, landing in pending:
            copy.wait()
            target = acc if k < levels - 1 else gat
            rows = pl.ds(pl.multiple_of(keep_off, 8), part)
            target[rows, :] = acc[rows, :] + landing[...]
        dcopy.wait()
        dacc[k + 1] = dacc[k] + drecv[k]

    depth = max(len(t) for t in trail)
    for back in range(depth):
        pending = []
        for i in range(len(streams)):
            if back >= len(trail[i]):
                continue
            peer, _, keep_off, part = trail[i][len(trail[i]) - 1 - back]
            copy = pltpu.make_async_remote_copy(
                src_ref=at(gat, keep_off, part), dst_ref=at(gat, keep_off, part),
                send_sem=send_sem.at[i, levels + back], recv_sem=recv_sem.at[i, levels + back],
                device_id=(peer,), device_id_type=MESH,
            )
            copy.start()
            pending.append(copy)
        fill(2)
        for copy in pending:
            copy.wait()
    fill(len(steps))

    for j in range(width // LANES):
        total[:, j * LANES : (j + 1) * LANES] = gat[j * order : (j + 1) * order, :]
    tail(total, dacc.at[levels], r2, inv1, inv2, h, e, vh, vl, gram, second, third, bh, bl)


def alone_kernel(packed, diag, r1, r2, rg, vh, vl, bh, bl, inv1, inv2, w, h, e, gram, second, third):
    for step in small_steps(r1, r2, rg, inv1, inv2, w, h, e, vh, vl):
        step()
    tail(packed, diag, r2, inv1, inv2, h, e, vh, vl, gram, second, third, bh, bl)


def weights(n, packed, diag, r_first, r_second, r_grad):
    levels = n.bit_length() - 1
    width = r_first.shape[0]
    vmem = pl.BlockSpec(memory_space=pltpu.VMEM)
    square = pltpu.VMEM((width, width), jnp.float32)
    outs = (jax.ShapeDtypeStruct((width, width), jnp.bfloat16),) * 4
    if n != 1 << levels or n < 4:
        packed, diag = lax.psum((packed, diag), "rows")
        return pl.pallas_call(
            alone_kernel,
            out_shape=outs,
            in_specs=[vmem] * 5,
            out_specs=(vmem,) * 4,
            scratch_shapes=[square] * 8,
            compiler_params=pltpu.CompilerParams(vmem_limit_bytes=VMEM_BYTES),
            name="weights",
        )(packed, diag, r_first, r_second, r_grad)
    rows = packed.size // LANES
    return pl.pallas_call(
        functools.partial(reduce_kernel, n),
        out_shape=outs,
        in_specs=[vmem] * 5,
        out_specs=(vmem,) * 4,
        scratch_shapes=[square] * 9
        + [
            pltpu.VMEM((rows, LANES), jnp.float32),
            pltpu.VMEM((2 * rows, LANES), jnp.float32),
            pltpu.VMEM((rows, LANES), jnp.float32),
            pltpu.VMEM((levels + 1,) + diag.shape, jnp.float32),
            pltpu.VMEM((levels,) + diag.shape, jnp.float32),
            pltpu.SemaphoreType.DMA((3, 2 * levels)),
            pltpu.SemaphoreType.DMA((3, 2 * levels)),
            pltpu.SemaphoreType.DMA((levels,)),
            pltpu.SemaphoreType.DMA((levels,)),
        ],
        compiler_params=pltpu.CompilerParams(
            collective_id=0, has_side_effects=True, vmem_limit_bytes=VMEM_BYTES
        ),
        name="weights",
    )(packed, diag, r_first, r_second, r_grad)


def tile_of(rows):
    for tile in (512, 384, 256, 128, 64, 32, 16):
        if rows % tile == 0:
            return tile
    return rows


def local(n, q_final, r_first, r_second, q_grad, r_grad):
    rows, width = q_final.shape
    tile = tile_of(rows)
    rowspec = pl.BlockSpec((tile, width), lambda i: (i, 0))
    fixed = pl.BlockSpec((width, width), lambda i: (0, 0))
    packed, diag = pl.pallas_call(
        gram_kernel,
        grid=(rows // tile,),
        out_shape=(
            jax.ShapeDtypeStruct((width, width), jnp.float32),
            jax.ShapeDtypeStruct((8, width), jnp.float32),
        ),
        in_specs=[rowspec, rowspec],
        out_specs=(fixed, pl.BlockSpec((8, width), lambda i: (0, 0))),
        scratch_shapes=[pltpu.VMEM((width, width), jnp.float32)] * 2,
        compiler_params=pltpu.CompilerParams(vmem_limit_bytes=VMEM_BYTES),
        name="grams",
    )(q_final, q_grad)
    split_weights = weights(n, packed, diag, r_first, r_second, r_grad)
    return pl.pallas_call(
        last_kernel,
        grid=(rows // tile,),
        out_shape=jax.ShapeDtypeStruct((rows, width), jnp.float32),
        in_specs=[rowspec, rowspec] + [fixed] * 4,
        out_specs=rowspec,
        compiler_params=pltpu.CompilerParams(vmem_limit_bytes=VMEM_BYTES),
        name="last",
    )(q_final, q_grad, *split_weights)


def solution(mesh):
    n = mesh.shape["rows"]
    placed = (P("rows", None), P(), P(), P("rows", None), P())
    return jax.shard_map(
        functools.partial(local, n), mesh=mesh, in_specs=placed, out_specs=P("rows", None), check_vma=False
    )
```

```python
import functools

import jax
import jax.numpy as jnp
from jax import lax
from jax.experimental import pallas as pl
from jax.experimental.pallas import tpu as pltpu
from jax.sharding import PartitionSpec as P

MESH = pl.DeviceIdType.MESH
LANES = 128
FULL_ROWS = 96
VMEM_BYTES = 56 * 1024 * 1024


def iota2(shape):
    return lax.broadcasted_iota(jnp.int32, shape, 0), lax.broadcasted_iota(jnp.int32, shape, 1)


def split(x):
    high = x.astype(jnp.bfloat16)
    return high, (x - high.astype(jnp.float32)).astype(jnp.bfloat16)


def mm(a, b, dims=((1,), (0,))):
    a_high, a_low = split(a)
    b_high, b_low = split(b)
    dot = functools.partial(
        lax.dot_general, dimension_numbers=(dims, ((), ())), preferred_element_type=jnp.float32
    )
    return dot(a_high, b_high) + (dot(a_high, b_low) + dot(a_low, b_high))


NT = ((1,), (1,))


TN = ((0,), (0,))


def inverse_steps(uppers, outs):
    order = uppers[0].shape[0]
    base = LANES if order % LANES == 0 else order
    spots = [(m, slice(s, s + base)) for m in range(len(uppers)) for s in range(0, order, base)]

    def init():
        row, col = iota2((base, base))
        eye = row == col
        for out in outs:
            out[...] = jnp.zeros_like(out)
        for m, s in spots:
            outs[m][s, s] = jnp.where(eye, 1.0 / jnp.where(eye, uppers[m][s, s], 1.0), 0.0)

    def inner(span):
        row, col = iota2((base, base))
        mask = (row // (2 * span) == col // (2 * span)) & (row // span < col // span)
        blocks = [outs[m][s, s] for m, s in spots]
        right = [mm(jnp.where(mask, uppers[m][s, s], 0.0), i) for (m, s), i in zip(spots, blocks)]
        for (m, s), i, r in zip(spots, blocks, right):
            outs[m][s, s] = i - mm(i, r)

    def corner(span):
        work = []
        for m in range(len(uppers)):
            for s in range(0, order - span, 2 * span):
                top, low = slice(s, s + span), slice(s + span, min(s + 2 * span, order))
                work.append((m, top, low, mm(uppers[m][top, low], outs[m][low, low])))
        for m, top, low, right in work:
            outs[m][top, low] = -mm(outs[m][top, top], right)

    steps, span = [init], 1
    while span < order:
        steps.append(functools.partial(inner if span < base else corner, span))
        span *= 2
    return steps


def small_steps(r1, r2, rg, inv1, inv2, w, h, e, vh, vl):
    def first():
        w[...] = mm(r1[...], rg[...], NT)

    def second():
        h[...] = mm(r2[...], w[...])

    def third():
        e[...] = mm(w[...], r2[...])

    def fourth():
        vh[...], vl[...] = split(mm(inv1[...], inv2[...]).T)

    return [first, second, third] + inverse_steps((r1, r2), (inv1, inv2)) + [fourth]


def copy_lower(matrix):
    row, col = iota2(matrix.shape)
    return jnp.where(row >= col, matrix, 0.0) + jnp.where(row > col, matrix, 0.0).T


def tail(packed, diag, r2, inv1, inv2, h, e, vh, vl, gram, second, third, bh, bl):
    row, col = iota2(packed.shape)
    upper = jnp.where(row < col, packed[...], 0.0)
    gram[...] = upper + upper.T + jnp.where(row == col, diag[0:1, :], 0.0)
    second[...] = copy_lower(h[...] - packed[...])
    third[...] = packed[...] + mm(second[...], gram[...])
    third[...] = mm(inv2[...], jnp.where(row >= col, third[...], 0.0))
    third[...] = copy_lower(e[...] - mm(third[...], r2[...]))
    third[...] = mm(r2[...], third[...])
    third[...] = mm(third[...], inv1[...], NT)
    s_high, s_low = split(second[...])
    dot = functools.partial(jnp.dot, preferred_element_type=jnp.float32)
    third[...] += dot(s_high, vh[...]) + (dot(s_high, vl[...]) + dot(s_low, vh[...]))
    bh[...], bl[...] = split(third[...])


def gram_kernel(q_ref, g_ref, out_ref, diag_ref, cross, gram):
    step = pl.program_id(0)

    @pl.when(step == 0)
    def _():
        cross[...] = jnp.zeros_like(cross)
        gram[...] = jnp.zeros_like(gram)

    half = q_ref.shape[1] // 2
    low, top = slice(0, half), slice(half, 2 * half)
    q1, q2, g1, g2 = q_ref[:, low], q_ref[:, top], g_ref[:, low], g_ref[:, top]
    q1, q2, g1, g2 = split(q1), split(q2), split(g1), split(g2)

    def product(a, b):
        dot = functools.partial(
            lax.dot_general, dimension_numbers=(TN, ((), ())), preferred_element_type=jnp.float32
        )
        return dot(a[0], b[0]) + (dot(a[0], b[1]) + dot(a[1], b[0]))

    cross[low, low] += product(g1, q1)
    cross[top, low] += product(g2, q1)
    cross[top, top] += product(g2, q2)
    gram[low, low] += product(q1, q1)
    gram[low, top] += product(q1, q2)
    gram[top, top] += product(q2, q2)

    @pl.when(step == pl.num_programs(0) - 1)
    def _():
        row, col = iota2(out_ref.shape)
        out_ref[...] = jnp.where(row >= col, cross[...], gram[...])
        line = jnp.sum(jnp.where(row == col, gram[...], 0.0), axis=0, keepdims=True)
        diag_ref[...] = jnp.broadcast_to(line, diag_ref.shape)


def last_kernel(q_ref, g_ref, vh, vl, bh, bl, out_ref):
    g_high, g_low = split(g_ref[...])
    q_high, q_low = split(q_ref[...])
    dot = functools.partial(jnp.dot, preferred_element_type=jnp.float32)
    out_ref[...] = (dot(g_high, vh[...]) + dot(q_high, bh[...])) + (
        (dot(g_high, vl[...]) + dot(g_low, vh[...])) + (dot(q_high, bl[...]) + dot(q_low, bh[...]))
    )


def plan(n, rows):
    bits = list(range(n.bit_length() - 1))
    rest = bits[1:]
    half = len(rest) // 2
    swapped = [rest[i ^ 1] if (i ^ 1) < len(rest) else rest[i] for i in range(len(rest))]
    orders = [rest, swapped, rest[half:] + rest[:half]]
    unit = rows // 8
    sizes = [3 * unit, 3 * unit, rows - 6 * unit]
    out, start = [], 0
    for order, size in zip(orders, sizes):
        out.append((start, size, bits[:1] + order))
        start += size
    return out


def reduce_kernel(
    n, p_ref, d_ref, r1, r2, rg, vh, vl, bh, bl,
    total, inv1, inv2, w, h, e, gram, second, third,
    acc, recv, gat, dacc, drecv, send_sem, recv_sem, dsend, drecv_sem,
):
    me = lax.axis_index("rows")
    levels = n.bit_length() - 1
    order, width = p_ref.shape

    def partner(bit):
        step = 1 << bit
        return me + step * (1 - 2 * ((me // step) % 2))

    barrier = pltpu.get_barrier_semaphore()
    for bit in range(levels):
        pl.semaphore_signal(barrier, inc=1, device_id=(partner(bit),), device_id_type=MESH)
    pl.semaphore_wait(barrier, levels)

    for j in range(width // LANES):
        acc[j * order : (j + 1) * order, :] = p_ref[:, j * LANES : (j + 1) * LANES]
    dacc[0] = d_ref[...]

    streams = plan(n, acc.shape[0])
    steps = small_steps(r1, r2, rg, inv1, inv2, w, h, e, vh, vl)

    def fill(count):
        for _ in range(min(count, len(steps))):
            steps.pop(0)()

    state = [(start, size) for start, size, _ in streams]
    base = [0] * len(streams)
    slot0 = 0
    for i, (_, size, _) in enumerate(streams):
        base[i] = slot0
        slot0 += 2 * size
    trail = [[] for _ in streams]

    def at(ref, off, size):
        return ref.at[pl.ds(pl.multiple_of(off, 8), size), :]

    for k in range(levels):
        pending = []
        for i, (_, _, bits) in enumerate(streams):
            off, size = state[i]
            peer = partner(bits[k])
            mine = (me // (1 << bits[k])) % 2
            halve = (size // 2) % 8 == 0 and size > FULL_ROWS
            part = size // 2 if halve else size
            send_off = off + (1 - mine) * part if halve else off
            keep_off = off + mine * part if halve else off
            landing = recv.at[pl.ds(base[i], part), :]
            copy = pltpu.make_async_remote_copy(
                src_ref=at(acc, send_off, part), dst_ref=landing,
                send_sem=send_sem.at[i, k], recv_sem=recv_sem.at[i, k],
                device_id=(peer,), device_id_type=MESH,
            )
            copy.start()
            pending.append((i, copy, keep_off, part, landing))
            if halve:
                trail[i].append((peer, off, keep_off, part))
            base[i] += part
            state[i] = (keep_off, part)
        dcopy = pltpu.make_async_remote_copy(
            src_ref=dacc.at[k], dst_ref=drecv.at[k], send_sem=dsend.at[k], recv_sem=drecv_sem.at[k],
            device_id=(partner(k),), device_id_type=MESH,
        )
        dcopy.start()
        fill(2)
        for i, copy, keep_off, part, landing in pending:
            copy.wait()
            target = acc if k < levels - 1 else gat
            rows = pl.ds(pl.multiple_of(keep_off, 8), part)
            target[rows, :] = acc[rows, :] + landing[...]
        dcopy.wait()
        dacc[k + 1] = dacc[k] + drecv[k]

    depth = max(len(t) for t in trail)
    for back in range(depth):
        pending = []
        for i in range(len(streams)):
            if back >= len(trail[i]):
                continue
            peer, _, keep_off, part = trail[i][len(trail[i]) - 1 - back]
            copy = pltpu.make_async_remote_copy(
                src_ref=at(gat, keep_off, part), dst_ref=at(gat, keep_off, part),
                send_sem=send_sem.at[i, levels + back], recv_sem=recv_sem.at[i, levels + back],
                device_id=(peer,), device_id_type=MESH,
            )
            copy.start()
            pending.append(copy)
        fill(2)
        for copy in pending:
            copy.wait()
    fill(len(steps))

    for j in range(width // LANES):
        total[:, j * LANES : (j + 1) * LANES] = gat[j * order : (j + 1) * order, :]
    tail(total, dacc.at[levels], r2, inv1, inv2, h, e, vh, vl, gram, second, third, bh, bl)


def alone_kernel(packed, diag, r1, r2, rg, vh, vl, bh, bl, inv1, inv2, w, h, e, gram, second, third):
    for step in small_steps(r1, r2, rg, inv1, inv2, w, h, e, vh, vl):
        step()
    tail(packed, diag, r2, inv1, inv2, h, e, vh, vl, gram, second, third, bh, bl)


def weights(n, packed, diag, r_first, r_second, r_grad):
    levels = n.bit_length() - 1
    width = r_first.shape[0]
    vmem = pl.BlockSpec(memory_space=pltpu.VMEM)
    square = pltpu.VMEM((width, width), jnp.float32)
    outs = (jax.ShapeDtypeStruct((width, width), jnp.bfloat16),) * 4
    if n != 1 << levels or n < 4:
        packed, diag = lax.psum((packed, diag), "rows")
        return pl.pallas_call(
            alone_kernel,
            out_shape=outs,
            in_specs=[vmem] * 5,
            out_specs=(vmem,) * 4,
            scratch_shapes=[square] * 8,
            compiler_params=pltpu.CompilerParams(vmem_limit_bytes=VMEM_BYTES),
            name="weights",
        )(packed, diag, r_first, r_second, r_grad)
    rows = packed.size // LANES
    return pl.pallas_call(
        functools.partial(reduce_kernel, n),
        out_shape=outs,
        in_specs=[vmem] * 5,
        out_specs=(vmem,) * 4,
        scratch_shapes=[square] * 9
        + [
            pltpu.VMEM((rows, LANES), jnp.float32),
            pltpu.VMEM((2 * rows, LANES), jnp.float32),
            pltpu.VMEM((rows, LANES), jnp.float32),
            pltpu.VMEM((levels + 1,) + diag.shape, jnp.float32),
            pltpu.VMEM((levels,) + diag.shape, jnp.float32),
            pltpu.SemaphoreType.DMA((3, 2 * levels)),
            pltpu.SemaphoreType.DMA((3, 2 * levels)),
            pltpu.SemaphoreType.DMA((levels,)),
            pltpu.SemaphoreType.DMA((levels,)),
        ],
        compiler_params=pltpu.CompilerParams(
            collective_id=0, has_side_effects=True, vmem_limit_bytes=VMEM_BYTES
        ),
        name="weights",
    )(packed, diag, r_first, r_second, r_grad)


def tile_of(rows):
    for tile in (256, 128, 64, 32, 16):
        if rows % tile == 0:
            return tile
    return rows


def local(n, q_final, r_first, r_second, q_grad, r_grad):
    rows, width = q_final.shape
    tile = tile_of(rows)
    rowspec = pl.BlockSpec((tile, width), lambda i: (i, 0))
    fixed = pl.BlockSpec((width, width), lambda i: (0, 0))
    packed, diag = pl.pallas_call(
        gram_kernel,
        grid=(rows // tile,),
        out_shape=(
            jax.ShapeDtypeStruct((width, width), jnp.float32),
            jax.ShapeDtypeStruct((8, width), jnp.float32),
        ),
        in_specs=[rowspec, rowspec],
        out_specs=(fixed, pl.BlockSpec((8, width), lambda i: (0, 0))),
        scratch_shapes=[pltpu.VMEM((width, width), jnp.float32)] * 2,
        compiler_params=pltpu.CompilerParams(vmem_limit_bytes=VMEM_BYTES),
        name="grams",
    )(q_final, q_grad)
    split_weights = weights(n, packed, diag, r_first, r_second, r_grad)
    return pl.pallas_call(
        last_kernel,
        grid=(rows // tile,),
        out_shape=jax.ShapeDtypeStruct((rows, width), jnp.float32),
        in_specs=[rowspec, rowspec] + [fixed] * 4,
        out_specs=rowspec,
        compiler_params=pltpu.CompilerParams(vmem_limit_bytes=VMEM_BYTES),
        name="last",
    )(q_final, q_grad, *split_weights)


def solution(mesh):
    n = mesh.shape["rows"]
    placed = (P("rows", None), P(), P(), P("rows", None), P())
    return jax.shard_map(
        functools.partial(local, n), mesh=mesh, in_specs=placed, out_specs=P("rows", None), check_vma=False
    )
```
